128 devices in a mesh: freq: 16 (over y, z_lo, core), feed: 8 (over z_hi, x).
Axes of the slice: x: 4, y: 4, z: 4 (z_hi: 2, z_lo: 2; z = z_hi * 2 + z_lo), core: 2. Of those that a mesh axis runs over, the one named last changes fastest.
Arguments:
- voltages: int32 [64, 2048, 2, 768], P(None, ('feed', 'freq')), may hold values from -127 to 127
- gains: float32 [2, 64, 2048], P(None, None, ('feed', 'freq')), may hold values from -0.06 to 0.06
Outputs:
- visibilities: float32 [64, 2, 2048, 2048], P('freq', None, 'feed')
The draws below stay inside these ranges and needn't reach their ends.
All inputs are finite; a program needn't handle non-finite values.
Results may differ from the reference program's by a relative error of at most 0.0031.
Values may be sent and summed in bfloat16 or wider, within the bound.
A program may use at most 192 MiB of HBM per device.

```python
import jax
import jax.numpy as jnp
from jax import lax

FEEDS = 2048
TIME = 768
CHAN = 64


def set_ends(array, rng, low, top_value):
    place = [jax.random.randint(jax.random.fold_in(rng, axis), (), 0, length) for axis, length in enumerate(array.shape)]
    longest = array.shape.index(max(array.shape))
    beside = place[:longest] + [(place[longest] + 1) % array.shape[longest]] + place[longest + 1:]
    return array.at[tuple(place)].set(low).at[tuple(beside)].set(top_value)


def block_scale(rng, dims, shards, least, top_value):
    loudness = 1.0
    for position, blocks in shards:
        draws = jax.random.uniform(jax.random.fold_in(jax.random.fold_in(rng, 6), position), (blocks,), jnp.float32, least / len(shards), top_value / len(shards))
        loudness = loudness * jnp.repeat(jnp.exp(draws), dims[position] // blocks).reshape((-1,) + (1,) * (len(dims) - 1 - position))
    return loudness


def gaussian(rng, dims, scale, limit, cuts=(), held_as=jnp.bfloat16):
    values = scale * jax.random.normal(rng, dims, jnp.float32)
    if cuts:
        values = values * block_scale(rng, dims, cuts, -0.22, 0.18)
    return jnp.clip(values, -limit, limit).astype(held_as)


def setup_inputs(seed: int = 0) -> dict:
    key_list = jax.random.split(jax.random.key(seed), 3)
    voltages = set_ends(jax.random.randint(key_list[0], (CHAN, FEEDS, 2, TIME), -127, 128), jax.random.fold_in(key_list[0], 1), -127, 127).astype(jnp.int32)
    gains = gaussian(key_list[1], (2, CHAN, FEEDS), 0.01, 0.06, ((2, 128),), jnp.float32)
    return {"voltages": voltages, "gains": gains}


def reference(voltages, gains):
    volt_real = voltages[:, :, 0, :].astype(jnp.float32)
    volt_imag = voltages[:, :, 1, :].astype(jnp.float32)
    gain_real = gains[0][:, :, None]
    gain_imag = gains[1][:, :, None]
    eq_real = gain_real * volt_real - gain_imag * volt_imag
    eq_imag = gain_real * volt_imag + gain_imag * volt_real
    equalized = jnp.stack([eq_real, eq_imag], axis=2).astype(jnp.bfloat16)

    def per_channel(block):
        columns = block.reshape(FEEDS, 2 * TIME)
        swapped = jnp.concatenate([block[:, 1, :], -block[:, 0, :]], axis=1)
        left_side = jnp.concatenate([columns, swapped], axis=0)
        result = jnp.dot(left_side, columns.T, preferred_element_type=jnp.float32)
        return result.reshape(2, FEEDS, FEEDS) * (1.0 / TIME)

    return lax.map(per_channel, equalized)
```

```python
import functools

import jax
import jax.numpy as jnp
from jax import lax
from jax.experimental import pallas as pl
from jax.experimental.pallas import tpu as pltpu
from jax.sharding import PartitionSpec as P

MESH = pl.DeviceIdType.MESH
PLANES, PLACES, CORES, ROW = 8, 8, 2, 4


def place():
    freq, feed = lax.axis_index("freq"), lax.axis_index("feed")
    return freq // 2, freq % 2, feed


def chip_at(plane, feed, dx, dy, dz):
    z = (feed // ROW * 2 + plane % 2 + dz) % 4
    y = (plane // 2 + dy) % 4
    x = (feed % ROW + dx) % 4
    return y * 2 + z % 2, z // 2 * ROW + x


def offset_of(step):
    a, b = step // 4 % 4, step % 4
    return a, b, (step // 16 - a - b + 8) % 4


def kernel(volt, gains, arrived, raw, eq, samples, tiles, raw_sem, eq_send, eq_recv, pair_send, pair_recv, out_send, out_recv):
    plane, core, feed = place()
    chans, rows, _, time = volt.shape
    block = rows * PLANES * CORES
    half = block * PLACES // CORES
    me = feed * block + (plane * CORES + core) * rows

    def raw_copy(step):
        p, f = chip_at(plane, feed, *offset_of(step))
        return pltpu.make_async_copy(volt.at[p * PLACES + f], raw.at[step], raw_sem.at[step])

    def start_raw(step, carry):
        raw_copy(step).start()
        return carry

    lax.fori_loop(0, chans, start_raw, 0)

    def eq_copy(step):
        p, f = chip_at(plane, feed, *offset_of(step))
        return pltpu.make_async_remote_copy(
            eq.at[pl.ds(step * rows, rows)], samples.at[pl.ds(me, rows)], eq_send, eq_recv.at[feed],
            device_id={"freq": p * CORES + core, "feed": f}, device_id_type=MESH)

    own_copy = pltpu.make_async_copy(eq.at[pl.ds(0, rows)], samples.at[pl.ds(me, rows)], eq_recv.at[feed])
    lanes = lax.broadcasted_iota(jnp.int32, (rows, 2 * chans), 1)

    def equalize(step, carry):
        raw_copy(step).wait()
        p, f = chip_at(plane, feed, *offset_of(step))
        chan = p * PLACES + f
        g = gains[...]
        gr = jnp.sum(jnp.where(lanes == chan, g, 0.0), axis=1, keepdims=True)
        gi = jnp.sum(jnp.where(lanes == chan + chans, g, 0.0), axis=1, keepdims=True)
        vr = raw[step, :, 0, :].astype(jnp.float32)
        vi = raw[step, :, 1, :].astype(jnp.float32)
        eq[pl.ds(step * rows, rows), :time] = (gr * vr - gi * vi).astype(jnp.bfloat16)
        eq[pl.ds(step * rows, rows), time:] = (gr * vi + gi * vr).astype(jnp.bfloat16)

        @pl.when(step == 1)
        def _():
            own_copy.start()

        @pl.when(step > 1)
        def _():
            eq_copy(step - 1).start()
        return carry

    lax.fori_loop(0, chans, equalize, 0)
    eq_copy(chans - 1).start()

    def pair_copy(f, p):
        at = f * block + (p * CORES + core) * rows
        return pltpu.make_async_remote_copy(
            samples.at[pl.ds(at, rows)], samples.at[pl.ds(at, rows)], pair_send, pair_recv.at[f],
            device_id={"freq": plane * CORES + 1 - core}, device_id_type=MESH)

    def whole(ref, sem):
        return pltpu.make_async_copy(ref, ref, sem)

    def pass_on(f, carry):
        whole(samples.at[pl.ds(0, PLANES * rows)], eq_recv.at[f]).wait()

        def one(p, carry):
            pair_copy(f, p).start()
            return carry
        return lax.fori_loop(0, PLANES, one, carry)

    lax.fori_loop(0, PLACES, pass_on, 0)

    def pair_wait(f, carry):
        whole(samples.at[pl.ds(0, PLANES * rows)], pair_recv.at[f]).wait()
        return carry

    lax.fori_loop(0, PLACES, pair_wait, 0)

    owner = feed // ROW
    slot = feed % ROW
    cols = block
    per_place = half // cols

    def dest(step):
        i = step % PLACES
        dx = i // 2
        dz = i % 2
        return (feed // ROW + dz) % 2 * ROW + (feed % ROW + dx) % 4, step // PLACES

    def tile_ends(step, part):
        to, col = dest(step)
        src = tiles.at[to, part, :, pl.ds(pl.multiple_of(col * cols, cols), cols)]
        dst = arrived.at[slot, part, :, pl.ds(pl.multiple_of(core * half + col * cols, cols), cols)]
        return to, src, dst

    def send(step):
        for part in range(2):
            to, src, dst = tile_ends(step, part)
            far = pltpu.make_async_remote_copy(
                src, dst, out_send, out_recv.at[slot * CORES + core],
                device_id={"freq": plane * CORES + owner, "feed": to}, device_id_type=MESH)
            near = pltpu.make_async_copy(src, dst, out_recv.at[slot * CORES + core])
            here = jnp.logical_and(to == feed, owner == core)

            @pl.when(here)
            def _():
                near.start()

            @pl.when(jnp.logical_not(here))
            def _():
                far.start()

    def correlate(step, carry):
        to, col = dest(step)
        own = samples[pl.ds(pl.multiple_of(to * block, block), block), :]
        turned = jnp.concatenate([own[:, time:], -own[:, :time]], axis=1)
        left = jnp.concatenate([own, turned], axis=0)
        right = samples[pl.ds(pl.multiple_of(core * half + col * cols, cols), cols), :]
        product = lax.dot_general(left, right, (((1,), (1,)), ((), ())), preferred_element_type=jnp.float32)
        product = (product * (1.0 / time)).astype(jnp.bfloat16)
        at = pl.ds(pl.multiple_of(col * cols, cols), cols)
        tiles[to, 0, :, at] = product[:block]
        tiles[to, 1, :, at] = product[block:]

        @pl.when(step > 0)
        def _():
            send(step - 1)
        return carry

    steps = PLACES * per_place
    lax.fori_loop(0, steps, correlate, 0)
    send(steps - 1)

    def landed(i, carry):
        ref = arrived.at[i // CORES, :, :, pl.ds(pl.multiple_of(i % CORES * half, half), half)]
        whole(ref, out_recv.at[i]).wait()
        return carry

    lax.fori_loop(0, ROW * CORES, landed, 0)
    whole(eq.at[pl.ds(0, (chans - 1) * rows)], eq_send).wait()
    whole(samples.at[pl.ds(0, half)], pair_send).wait()

    def sent(i, carry):
        whole(tiles.at[0], out_send).wait()
        return carry

    lax.fori_loop(0, PLACES - 1, sent, 0)

    @pl.when(owner != core)
    def _():
        whole(tiles.at[0], out_send).wait()


def per_device(voltages, gains):
    chans, rows, _, time = voltages.shape
    feeds = rows * PLANES * CORES * PLACES
    block = feeds // PLACES
    owned = chans // (PLANES * CORES)
    flat = gains.transpose(2, 0, 1).reshape(rows, 2 * chans)
    arrived = pl.pallas_call(
        kernel,
        out_shape=jax.ShapeDtypeStruct((owned, 2, block, feeds), jnp.bfloat16),
        in_specs=[pl.BlockSpec(memory_space=pl.ANY), pl.BlockSpec(memory_space=pltpu.VMEM)],
        out_specs=pl.BlockSpec(memory_space=pl.ANY),
        scratch_shapes=[
            pltpu.VMEM((chans, rows, 2, time), jnp.int32),
            pltpu.VMEM((chans * rows, 2 * time), jnp.bfloat16),
            pltpu.VMEM((feeds, 2 * time), jnp.bfloat16),
            pltpu.VMEM((PLACES, 2, block, feeds // CORES), jnp.bfloat16),
            pltpu.SemaphoreType.DMA((chans,)),
            pltpu.SemaphoreType.DMA,
            pltpu.SemaphoreType.DMA((PLACES,)),
            pltpu.SemaphoreType.DMA,
            pltpu.SemaphoreType.DMA((PLACES,)),
            pltpu.SemaphoreType.DMA,
            pltpu.SemaphoreType.DMA((ROW * CORES,)),
        ],
        compiler_params=pltpu.CompilerParams(has_side_effects=True, vmem_limit_bytes=60 * 2**20),
        name="x_engine",
    )(voltages, flat)
    return arrived.astype(jnp.float32)


def solution(mesh):
    in_specs = (P(None, ("feed", "freq"), None, None), P(None, None, ("feed", "freq")))
    out_specs = P("freq", None, "feed", None)
    return jax.shard_map(
        per_device, mesh=mesh, in_specs=in_specs, out_specs=out_specs, check_vma=False
    )
```

```python
import functools

import jax
import jax.numpy as jnp
from jax import lax
from jax.experimental import pallas as pl
from jax.experimental.pallas import tpu as pltpu
from jax.sharding import PartitionSpec as P

MESH = pl.DeviceIdType.MESH
PLANES, PLACES, CORES, ROW = 8, 8, 2, 4


def place():
    freq, feed = lax.axis_index("freq"), lax.axis_index("feed")
    return freq // 2, freq % 2, feed


def chip_at(plane, feed, dx, dy, dz):
    z = (feed // ROW * 2 + plane % 2 + dz) % 4
    y = (plane // 2 + dy) % 4
    x = (feed % ROW + dx) % 4
    return y * 2 + z % 2, z // 2 * ROW + x


def offset_of(step):
    a, b = step // 4 % 4, step % 4
    return a, b, (step // 16 - a - b + 8) % 4


def kernel(volt, gains, arrived, raw, eq, samples, tiles, raw_sem, eq_send, eq_recv, pair_send, pair_recv, out_send, out_recv):
    plane, core, feed = place()
    chans, rows, _, time = volt.shape
    block = rows * PLANES * CORES
    half = block * PLACES // CORES
    me = feed * block + (plane * CORES + core) * rows

    def raw_copy(step):
        p, f = chip_at(plane, feed, *offset_of(step))
        return pltpu.make_async_copy(volt.at[p * PLACES + f], raw.at[step], raw_sem.at[step])

    def start_raw(step, carry):
        raw_copy(step).start()
        return carry

    lax.fori_loop(0, chans, start_raw, 0)

    barrier = pltpu.get_barrier_semaphore()

    def greet(step, carry):
        p, f = chip_at(plane, feed, *offset_of(step))
        pl.semaphore_signal(barrier, inc=1, device_id={"freq": p * CORES + core, "feed": f}, device_id_type=MESH)
        return carry

    def greet_other(f, carry):
        pl.semaphore_signal(barrier, inc=1, device_id={"freq": plane * CORES + 1 - core, "feed": f}, device_id_type=MESH)
        return carry

    lax.fori_loop(1, chans, greet, 0)
    lax.fori_loop(0, PLACES, greet_other, 0)

    def eq_copy(step):
        p, f = chip_at(plane, feed, *offset_of(step))
        return pltpu.make_async_remote_copy(
            eq.at[pl.ds(step * rows, rows)], samples.at[pl.ds(me, rows)], eq_send, eq_recv.at[feed],
            device_id={"freq": p * CORES + core, "feed": f}, device_id_type=MESH)

    own_copy = pltpu.make_async_copy(eq.at[pl.ds(0, rows)], samples.at[pl.ds(me, rows)], eq_recv.at[feed])
    lanes = lax.broadcasted_iota(jnp.int32, (rows, chans), 1)

    def equalize(step, carry):
        raw_copy(step).wait()
        p, f = chip_at(plane, feed, *offset_of(step))
        chan = p * PLACES + f
        gr = jnp.sum(jnp.where(lanes == chan, gains[0], 0.0), axis=1, keepdims=True)
        gi = jnp.sum(jnp.where(lanes == chan, gains[1], 0.0), axis=1, keepdims=True)
        vr = raw[step, :, 0, :].astype(jnp.float32)
        vi = raw[step, :, 1, :].astype(jnp.float32)
        eq[pl.ds(step * rows, rows), :time] = (gr * vr - gi * vi).astype(jnp.bfloat16)
        eq[pl.ds(step * rows, rows), time:] = (gr * vi + gi * vr).astype(jnp.bfloat16)
        return carry

    lax.fori_loop(0, chans, equalize, 0)
    pl.semaphore_wait(barrier, chans - 1 + PLACES)
    own_copy.start()

    def send_eq(step, carry):
        eq_copy(step).start()
        return carry

    lax.fori_loop(1, chans, send_eq, 0)

    def pair_copy(f, p):
        at = f * block + (p * CORES + core) * rows
        return pltpu.make_async_remote_copy(
            samples.at[pl.ds(at, rows)], samples.at[pl.ds(at, rows)], pair_send, pair_recv.at[f],
            device_id={"freq": plane * CORES + 1 - core}, device_id_type=MESH)

    def whole(ref, sem):
        return pltpu.make_async_copy(ref, ref, sem)

    row_x, row_z = feed % ROW, feed // ROW

    def near_place(dx, dz):
        return (row_z + dz) % 2 * ROW + (row_x + dx) % ROW

    def exchange(odd):
        def pass_on(i, carry):
            f = near_place(odd + i // 2 * 2, i % 2)
            whole(samples.at[pl.ds(0, PLANES * rows)], eq_recv.at[f]).wait()

            def one(p, carry):
                pair_copy(f, p).start()
                return carry
            return lax.fori_loop(0, PLANES, one, carry)

        def pair_wait(i, carry):
            f = near_place(odd + i // 2 * 2, i % 2)
            whole(samples.at[pl.ds(0, PLANES * rows)], pair_recv.at[f]).wait()
            return carry

        lax.fori_loop(0, PLACES // 2, pass_on, 0)
        lax.fori_loop(0, PLACES // 2, pair_wait, 0)

    owner, slot, cols = row_z, row_x, block

    def send(to, col):
        for part in range(2):
            src = tiles.at[to, part, :, pl.ds(pl.multiple_of(col * cols, cols), cols)]
            dst = arrived.at[slot, part, :, pl.ds(pl.multiple_of(core * half + col * cols, cols), cols)]
            far = pltpu.make_async_remote_copy(
                src, dst, out_send, out_recv.at[slot * CORES + core],
                device_id={"freq": plane * CORES + owner, "feed": to}, device_id_type=MESH)
            near = pltpu.make_async_copy(src, dst, out_recv.at[slot * CORES + core])
            here = jnp.logical_and(to == feed, owner == core)

            @pl.when(here)
            def _():
                near.start()

            @pl.when(jnp.logical_not(here))
            def _():
                far.start()

    def correlate(to, col):
        own = samples[pl.ds(pl.multiple_of(to * block, block), block), :]
        turned = jnp.concatenate([own[:, time:], -own[:, :time]], axis=1)
        left = jnp.concatenate([own, turned], axis=0)
        right = samples[pl.ds(pl.multiple_of(core * half + col * cols, cols), cols), :]
        product = lax.dot_general(left, right, (((1,), (1,)), ((), ())), preferred_element_type=jnp.float32)
        product = (product * (1.0 / time)).astype(jnp.bfloat16)
        at = pl.ds(pl.multiple_of(col * cols, cols), cols)
        tiles[to, 0, :, at] = product[:block]
        tiles[to, 1, :, at] = product[block:]

    def tile_loop(steps, tile):
        def one(step, carry):
            correlate(*tile(step))

            @pl.when(step > 0)
            def _():
                send(*tile(step - 1))
            return carry

        lax.fori_loop(0, steps, one, 0)
        send(*tile(steps - 1))

    def even_tile(step):
        i = step % 4
        return near_place(2 - i // 2 * 2, 1 - i % 2), (row_x + step // 4 * 2) % ROW

    def other_tile(step):
        turn, i = step // 6, step % 6
        odd = i < 4
        dx = jnp.where(odd, 3 - i % 2 * 2, 2 - turn % 2 * 2)
        dz = jnp.where(odd, 1 - i // 2, 5 - i)
        col = jnp.where(odd, turn, 1 + turn // 2 * 2)
        return near_place(dx, dz), (row_x + col) % ROW

    exchange(0)
    exchange(1)
    tile_loop(8, even_tile)
    tile_loop(24, other_tile)

    def landed(i, carry):
        ref = arrived.at[i // CORES, :, :, pl.ds(pl.multiple_of(i % CORES * half, half), half)]
        whole(ref, out_recv.at[i]).wait()
        return carry

    lax.fori_loop(0, ROW * CORES, landed, 0)
    whole(eq.at[pl.ds(0, (chans - 1) * rows)], eq_send).wait()
    whole(samples.at[pl.ds(0, half)], pair_send).wait()

    def sent(i, carry):
        whole(tiles.at[0], out_send).wait()
        return carry

    lax.fori_loop(0, PLACES - 1, sent, 0)

    @pl.when(owner != core)
    def _():
        whole(tiles.at[0], out_send).wait()


def per_device(voltages, gains):
    chans, rows, _, time = voltages.shape
    feeds = rows * PLANES * CORES * PLACES
    block = feeds // PLACES
    owned = chans // (PLANES * CORES)
    arrived = pl.pallas_call(
        kernel,
        out_shape=jax.ShapeDtypeStruct((owned, 2, block, feeds), jnp.bfloat16),
        in_specs=[pl.BlockSpec(memory_space=pl.ANY), pl.BlockSpec(memory_space=pltpu.VMEM)],
        out_specs=pl.BlockSpec(memory_space=pl.ANY),
        scratch_shapes=[
            pltpu.VMEM((chans, rows, 2, time), jnp.int32),
            pltpu.VMEM((chans * rows, 2 * time), jnp.bfloat16),
            pltpu.VMEM((feeds, 2 * time), jnp.bfloat16),
            pltpu.VMEM((PLACES, 2, block, feeds // CORES), jnp.bfloat16),
            pltpu.SemaphoreType.DMA((chans,)),
            pltpu.SemaphoreType.DMA,
            pltpu.SemaphoreType.DMA((PLACES,)),
            pltpu.SemaphoreType.DMA,
            pltpu.SemaphoreType.DMA((PLACES,)),
            pltpu.SemaphoreType.DMA,
            pltpu.SemaphoreType.DMA((ROW * CORES,)),
        ],
        compiler_params=pltpu.CompilerParams(collective_id=0, has_side_effects=True, vmem_limit_bytes=60 * 2**20),
        name="x_engine",
    )(voltages, gains.transpose(0, 2, 1))
    return arrived.astype(jnp.float32)


def solution(mesh):
    in_specs = (P(None, ("feed", "freq"), None, None), P(None, None, ("feed", "freq")))
    out_specs = P("freq", None, "feed", None)
    return jax.shard_map(
        per_device, mesh=mesh, in_specs=in_specs, out_specs=out_specs, check_vma=False
    )
```

```python
import functools

import jax
import jax.numpy as jnp
from jax import lax
from jax.experimental import pallas as pl
from jax.experimental.pallas import tpu as pltpu
from jax.sharding import PartitionSpec as P

MESH = pl.DeviceIdType.MESH
PLANES, PLACES, CORES, ROW = 8, 8, 2, 4


RELAYS = (
    ((0, 3), (2, 1)), ((0, 1), (2, 1)), ((0, 2), (2, 1)), ((0, 1), (1, 1)), ((0, 3), (3, 1)), ((0, 1), (2, 0)), ((0, 3), (2, 0)),
    ((1, 0), (2, 1)), ((1, 1), (2, 1)), ((1, 3), (2, 1)), ((1, 0), (1, 1)), ((1, 0), (3, 1)),
)
TILES = (
    ((1, 0, 2), (3, 0, 2), (2, 1, 0), (1, 1, 0), (3, 1, 0), (2, 0, 0), (0, 1, 0), (1, 0, 0), (3, 0, 0), (0, 0, 0), (1, 1, 2),
     (3, 1, 2), (0, 1, 1), (2, 0, 2), (1, 0, 1), (3, 0, 1), (0, 0, 1), (1, 1, 3), (3, 1, 1), (0, 1, 2), (1, 0, 3), (3, 0, 3),
     (0, 1, 3), (0, 0, 2), (0, 0, 3)),
    ((1, 0, 2), (3, 0, 2), (0, 1, 2), (2, 0, 2), (1, 1, 2), (3, 1, 2), (0, 1, 1), (1, 0, 1), (3, 0, 3), (0, 1, 3), (2, 1, 2),
     (1, 1, 1), (3, 1, 1), (2, 0, 0), (0, 1, 0), (1, 0, 0), (3, 0, 0), (0, 0, 0), (1, 1, 3), (3, 1, 3), (2, 0, 1), (1, 0, 3),
     (3, 0, 1), (0, 0, 1), (2, 0, 3), (0, 0, 2), (0, 0, 3)),
)


def pick(table, step):
    out = []
    for column in zip(*table):
        value = jnp.int32(column[0])
        for n in range(1, len(column)):
            value = jnp.where(step == n, column[n], value)
        out.append(value)
    return out


def relayed(giver_dz, giver_dx, taker_dx, taker_dz):
    hit = jnp.bool_(False)
    for (az, ax), (bx, bz) in RELAYS:
        same = (giver_dz == az) & (giver_dx == ax) & (taker_dx == bx) & (taker_dz == bz)
        hit = hit | same
    return hit


def place():
    freq, feed = lax.axis_index("freq"), lax.axis_index("feed")
    return freq // 2, freq % 2, feed


def chip_at(plane, feed, dx, dy, dz):
    z = (feed // ROW * 2 + plane % 2 + dz) % 4
    y = (plane // 2 + dy) % 4
    x = (feed % ROW + dx) % 4
    return y * 2 + z % 2, z // 2 * ROW + x


def offset_of(step):
    a, b = step // 4 % 4, step % 4
    return a, b, (step // 16 - a - b + 8) % 4


def kernel(volt, gains, arrived, raw, eq, samples, tiles, raw_sem, eq_send, eq_recv, pair_send, pair_recv, out_send, out_recv, relay_send):
    plane, core, feed = place()
    chans, rows, _, time = volt.shape
    block = rows * PLANES * CORES
    half = block * PLACES // CORES
    me = feed * block + (plane * CORES + core) * rows

    def raw_copy(step):
        p, f = chip_at(plane, feed, *offset_of(step))
        return pltpu.make_async_copy(volt.at[p * PLACES + f], raw.at[step], raw_sem.at[step])

    def start_raw(step, carry):
        raw_copy(step).start()
        return carry

    lax.fori_loop(0, chans, start_raw, 0)

    barrier = pltpu.get_barrier_semaphore()

    def greet(step, carry):
        p, f = chip_at(plane, feed, *offset_of(step))
        pl.semaphore_signal(barrier, inc=1, device_id={"freq": p * CORES + core, "feed": f}, device_id_type=MESH)
        return carry

    def greet_other(f, carry):
        pl.semaphore_signal(barrier, inc=1, device_id={"freq": plane * CORES + 1 - core, "feed": f}, device_id_type=MESH)
        return carry

    lax.fori_loop(1, chans, greet, 0)
    lax.fori_loop(0, PLACES, greet_other, 0)

    def eq_copy(step):
        p, f = chip_at(plane, feed, *offset_of(step))
        return pltpu.make_async_remote_copy(
            eq.at[pl.ds(step * rows, rows)], samples.at[pl.ds(me, rows)], eq_send, eq_recv.at[feed],
            device_id={"freq": p * CORES + core, "feed": f}, device_id_type=MESH)

    own_copy = pltpu.make_async_copy(eq.at[pl.ds(0, rows)], samples.at[pl.ds(me, rows)], eq_recv.at[feed])
    lanes = lax.broadcasted_iota(jnp.int32, (rows, chans), 1)

    def equalize(step, carry):
        raw_copy(step).wait()
        p, f = chip_at(plane, feed, *offset_of(step))
        chan = p * PLACES + f
        gr = jnp.sum(jnp.where(lanes == chan, gains[0], 0.0), axis=1, keepdims=True)
        gi = jnp.sum(jnp.where(lanes == chan, gains[1], 0.0), axis=1, keepdims=True)
        vr = raw[step, :, 0, :].astype(jnp.float32)
        vi = raw[step, :, 1, :].astype(jnp.float32)
        eq[pl.ds(step * rows, rows), :time] = (gr * vr - gi * vi).astype(jnp.bfloat16)
        eq[pl.ds(step * rows, rows), time:] = (gr * vi + gi * vr).astype(jnp.bfloat16)
        return carry

    lax.fori_loop(0, chans, equalize, 0)
    pl.semaphore_wait(barrier, chans - 1 + PLACES)
    own_copy.start()

    def send_eq(step, carry):
        eq_copy(step).start()
        return carry

    lax.fori_loop(1, chans, send_eq, 0)

    def pair_copy(f, p):
        at = f * block + (p * CORES + core) * rows
        return pltpu.make_async_remote_copy(
            samples.at[pl.ds(at, rows)], samples.at[pl.ds(at, rows)], pair_send, pair_recv.at[f],
            device_id={"freq": plane * CORES + 1 - core}, device_id_type=MESH)

    def whole(ref, sem):
        return pltpu.make_async_copy(ref, ref, sem)

    row_x, row_z = feed % ROW, feed // ROW

    def near_place(dx, dz):
        return (row_z + dz) % 2 * ROW + (row_x + dx) % ROW

    def exchange(odd):
        def pass_on(i, carry):
            f = near_place(odd + i // 2 * 2, i % 2)
            whole(samples.at[pl.ds(0, PLANES * rows)], eq_recv.at[f]).wait()

            def one(p, carry):
                pair_copy(f, p).start()
                return carry
            return lax.fori_loop(0, PLANES, one, carry)

        def pair_wait(i, carry):
            f = near_place(odd + i // 2 * 2, i % 2)
            whole(samples.at[pl.ds(0, PLANES * rows)], pair_recv.at[f]).wait()
            return carry

        lax.fori_loop(0, PLACES // 2, pass_on, 0)
        lax.fori_loop(0, PLACES // 2, pair_wait, 0)

    owner, slot, cols = row_z, row_x, block

    def send(to, col):
        for part in range(2):
            src = tiles.at[to, part, :, pl.ds(pl.multiple_of(col * cols, cols), cols)]
            dst = arrived.at[slot, part, :, pl.ds(pl.multiple_of(core * half + col * cols, cols), cols)]
            far = pltpu.make_async_remote_copy(
                src, dst, out_send, out_recv.at[slot, core * ROW + col],
                device_id={"freq": plane * CORES + owner, "feed": to}, device_id_type=MESH)
            near = pltpu.make_async_copy(src, dst, out_recv.at[slot, core * ROW + col])
            here = jnp.logical_and(to == feed, owner == core)

            @pl.when(here)
            def _():
                near.start()

            @pl.when(jnp.logical_not(here))
            def _():
                far.start()

    def correlate(to, col):
        own = samples[pl.ds(pl.multiple_of(to * block, block), block), :]
        turned = jnp.concatenate([own[:, time:], -own[:, :time]], axis=1)
        left = jnp.concatenate([own, turned], axis=0)
        right = samples[pl.ds(pl.multiple_of(core * half + col * cols, cols), cols), :]
        product = lax.dot_general(left, right, (((1,), (1,)), ((), ())), preferred_element_type=jnp.float32)
        product = (product * (1.0 / time)).astype(jnp.bfloat16)
        at = pl.ds(pl.multiple_of(col * cols, cols), cols)
        tiles[to, 0, :, at] = product[:block]
        tiles[to, 1, :, at] = product[block:]

    def tile_loop(steps, tile):
        def one(step, carry):
            correlate(*tile(step))

            @pl.when(step > 0)
            def _():
                send(*tile(step - 1))
            return carry

        lax.fori_loop(0, steps, one, 0)
        send(*tile(steps - 1))

    far_side = (core + row_z) % 2
    steps = len(TILES[0]) + far_side * (len(TILES[1]) - len(TILES[0]))

    def tile(step):
        close, far = pick(TILES[0], step), pick(TILES[1], step)
        dx, dz, col = (jnp.where(far_side == 1, v, u) for u, v in zip(close, far))
        return near_place(dx, dz), (row_x + col) % ROW

    exchange(0)
    exchange(1)
    tile_loop(steps, tile)

    def columns(source, f):
        return arrived.at[source, :, :, pl.ds(pl.multiple_of(f * cols, cols), cols)]

    near_relays = tuple((ax, bx, bz) for (az, ax), (bx, bz) in RELAYS if az == 0)
    far_relays = tuple((ax, bx, bz) for (az, ax), (bx, bz) in RELAYS if az == 1)
    relays = len(near_relays) + far_side * (len(far_relays) - len(near_relays))

    def hand_on(n, carry):
        ax, bx, bz = (jnp.where(far_side == 1, v, u) for u, v in zip(pick(near_relays, n), pick(far_relays, n)))
        source = (row_x - ax + ROW) % ROW
        to = (core + bz) % 2 * ROW + (source + bx) % ROW
        whole(columns(source, to), out_recv.at[source, to]).wait()
        pltpu.make_async_remote_copy(
            columns(source, to), columns(source, feed), relay_send, out_recv.at[source, feed],
            device_id={"freq": plane * CORES + core, "feed": to}, device_id_type=MESH).start()
        return carry

    lax.fori_loop(0, relays, hand_on, 0)

    def landed(i, carry):
        source, f = i // PLACES, i % PLACES
        seen = relayed(far_side, (row_x - source + ROW) % ROW, (f % ROW - source + ROW) % ROW, (f // ROW + core) % 2)

        @pl.when(jnp.logical_not(seen))
        def _():
            whole(columns(source, f), out_recv.at[source, f]).wait()
        return carry

    lax.fori_loop(0, ROW * PLACES, landed, 0)
    whole(eq.at[pl.ds(0, (chans - 1) * rows)], eq_send).wait()
    whole(samples.at[pl.ds(0, half)], pair_send).wait()
    one_tile = tiles.at[0, :, :, pl.ds(0, cols)]

    def sent(i, carry):
        whole(one_tile, out_send).wait()
        return carry

    lax.fori_loop(0, steps - jnp.where(owner == core, ROW, 0), sent, 0)

    def handed(i, carry):
        whole(one_tile, relay_send).wait()
        return carry

    lax.fori_loop(0, relays, handed, 0)


def finish(arrived, out):
    _, core, feed = place()
    source, width = pl.program_id(0), out.shape[2]
    for n in range(out.shape[3] // width):
        f = pl.program_id(1) * (out.shape[3] // width) + n
        turned = relayed((f // ROW + core) % 2, (f % ROW - source + ROW) % ROW,
                         (feed % ROW - source + ROW) % ROW, (feed // ROW + core) % 2)
        at = slice(n * width, (n + 1) * width)

        @pl.when(turned)
        def _():
            out[0, 0, :, at] = arrived[0, 0, :, at].astype(jnp.float32).T
            out[0, 1, :, at] = -arrived[0, 1, :, at].astype(jnp.float32).T

        @pl.when(jnp.logical_not(turned))
        def _():
            out[0, :, :, at] = arrived[0, :, :, at].astype(jnp.float32)


def per_device(voltages, gains):
    chans, rows, _, time = voltages.shape
    feeds = rows * PLANES * CORES * PLACES
    block = feeds // PLACES
    owned = chans // (PLANES * CORES)
    arrived = pl.pallas_call(
        kernel,
        out_shape=jax.ShapeDtypeStruct((owned, 2, block, feeds), jnp.bfloat16),
        in_specs=[pl.BlockSpec(memory_space=pl.ANY), pl.BlockSpec(memory_space=pltpu.VMEM)],
        out_specs=pl.BlockSpec(memory_space=pl.ANY),
        scratch_shapes=[
            pltpu.VMEM((chans, rows, 2, time), jnp.int32),
            pltpu.VMEM((chans * rows, 2 * time), jnp.bfloat16),
            pltpu.VMEM((feeds, 2 * time), jnp.bfloat16),
            pltpu.VMEM((PLACES, 2, block, feeds // CORES), jnp.bfloat16),
            pltpu.SemaphoreType.DMA((chans,)),
            pltpu.SemaphoreType.DMA,
            pltpu.SemaphoreType.DMA((PLACES,)),
            pltpu.SemaphoreType.DMA,
            pltpu.SemaphoreType.DMA((PLACES,)),
            pltpu.SemaphoreType.DMA,
            pltpu.SemaphoreType.DMA((ROW, PLACES)),
            pltpu.SemaphoreType.DMA,
        ],
        compiler_params=pltpu.CompilerParams(collective_id=0, has_side_effects=True, vmem_limit_bytes=60 * 2**20),
        name="x_engine",
    )(voltages, gains.transpose(0, 2, 1))
    spec = pl.BlockSpec((1, 2, block, feeds // 2), lambda i, j: (i, 0, 0, j))
    return pl.pallas_call(
        finish,
        out_shape=jax.ShapeDtypeStruct(arrived.shape, jnp.float32),
        grid=(owned, 2),
        in_specs=[spec],
        out_specs=spec,
        name="widen",
    )(arrived)


def solution(mesh):
    in_specs = (P(None, ("feed", "freq"), None, None), P(None, None, ("feed", "freq")))
    out_specs = P("freq", None, "feed", None)
    return jax.shard_map(
        per_device, mesh=mesh, in_specs=in_specs, out_specs=out_specs, check_vma=False
    )
```

```python
import functools

import jax
import jax.numpy as jnp
from jax import lax
from jax.experimental import pallas as pl
from jax.experimental.pallas import tpu as pltpu
from jax.sharding import PartitionSpec as P

MESH = pl.DeviceIdType.MESH
PLANES, PLACES, CORES, ROW = 8, 8, 2, 4


RELAYS = (
    ((0, 3), (2, 1)), ((0, 1), (2, 1)), ((0, 2), (2, 1)), ((0, 1), (1, 1)), ((0, 3), (3, 1)), ((0, 1), (2, 0)), ((0, 3), (2, 0)),
    ((1, 0), (2, 1)), ((1, 1), (2, 1)), ((1, 3), (2, 1)), ((1, 0), (1, 1)), ((1, 0), (3, 1)),
)
TILES = (
    ((1, 0, 2), (3, 0, 2), (0, 1, 0), (1, 1, 0), (3, 1, 0), (2, 0, 0), (1, 0, 0), (3, 0, 0), (0, 1, 1), (1, 1, 2), (3, 1, 1), (2, 1, 0), (1, 0, 1), (3, 0, 1), (0, 1, 2), (2, 0, 2), (1, 1, 3), (3, 1, 2), (1, 0, 3), (3, 0, 3), (0, 1, 3), (0, 0, 0), (0, 0, 1), (0, 0, 2), (0, 0, 3)),
    ((1, 0, 1), (3, 0, 2), (0, 1, 1), (2, 0, 2), (1, 1, 2), (3, 1, 2), (1, 0, 2), (3, 0, 3), (0, 1, 2), (2, 0, 0), (0, 1, 3), (1, 1, 1), (3, 1, 1), (2, 1, 2), (1, 0, 0), (3, 0, 0), (2, 0, 1), (1, 1, 3), (3, 1, 3), (1, 0, 3), (3, 0, 1), (0, 1, 0), (2, 0, 3), (0, 0, 0), (0, 0, 1), (0, 0, 2), (0, 0, 3)),
)


def pick(table, step):
    out = []
    for column in zip(*table):
        value = jnp.int32(column[0])
        for n in range(1, len(column)):
            value = jnp.where(step == n, column[n], value)
        out.append(value)
    return out


def relayed(giver_dz, giver_dx, taker_dx, taker_dz):
    hit = jnp.bool_(False)
    for (az, ax), (bx, bz) in RELAYS:
        same = (giver_dz == az) & (giver_dx == ax) & (taker_dx == bx) & (taker_dz == bz)
        hit = hit | same
    return hit


def place():
    freq, feed = lax.axis_index("freq"), lax.axis_index("feed")
    return freq // 2, freq % 2, feed


def chip_at(plane, feed, dx, dy, dz):
    z = (feed // ROW * 2 + plane % 2 + dz) % 4
    y = (plane // 2 + dy) % 4
    x = (feed % ROW + dx) % 4
    return y * 2 + z % 2, z // 2 * ROW + x


def offset_of(step):
    a, b = step // 4 % 4, step % 4
    return a, b, (step // 16 - a - b + 8) % 4


def kernel(volt, gains, arrived, raw, eq, samples, tiles, raw_sem, eq_send, eq_recv, pair_send, pair_recv, out_send, out_recv, relay_send):
    plane, core, feed = place()
    chans, rows, _, time = volt.shape
    block = rows * PLANES * CORES
    half = block * PLACES // CORES
    me = feed * block + (plane * CORES + core) * rows

    def raw_copy(step):
        p, f = chip_at(plane, feed, *offset_of(step))
        return pltpu.make_async_copy(volt.at[p * PLACES + f], raw.at[step], raw_sem.at[step])

    def start_raw(step, carry):
        raw_copy(step).start()
        return carry


    barrier = pltpu.get_barrier_semaphore()

    def greet(step, carry):
        p, f = chip_at(plane, feed, *offset_of(step))
        pl.semaphore_signal(barrier, inc=1, device_id={"freq": p * CORES + core, "feed": f}, device_id_type=MESH)
        return carry

    def greet_other(f, carry):
        pl.semaphore_signal(barrier, inc=1, device_id={"freq": plane * CORES + 1 - core, "feed": f}, device_id_type=MESH)
        return carry

    lax.fori_loop(1, chans, greet, 0)
    lax.fori_loop(0, PLACES, greet_other, 0)
    lax.fori_loop(0, chans, start_raw, 0)

    def eq_copy(step):
        p, f = chip_at(plane, feed, *offset_of(step))
        return pltpu.make_async_remote_copy(
            eq.at[pl.ds(step * rows, rows)], samples.at[pl.ds(me, rows)], eq_send, eq_recv.at[feed, plane],
            device_id={"freq": p * CORES + core, "feed": f}, device_id_type=MESH)

    own_copy = pltpu.make_async_copy(eq.at[pl.ds(0, rows)], samples.at[pl.ds(me, rows)], eq_recv.at[feed, plane])
    lanes = lax.broadcasted_iota(jnp.int32, (rows, chans), 1)

    def equalize(step, carry):
        raw_copy(step).wait()
        p, f = chip_at(plane, feed, *offset_of(step))
        chan = p * PLACES + f
        gr = jnp.sum(jnp.where(lanes == chan, gains[0], 0.0), axis=1, keepdims=True)
        gi = jnp.sum(jnp.where(lanes == chan, gains[1], 0.0), axis=1, keepdims=True)
        vr = raw[step, :, 0, :].astype(jnp.float32)
        vi = raw[step, :, 1, :].astype(jnp.float32)
        eq[pl.ds(step * rows, rows), :time] = (gr * vr - gi * vi).astype(jnp.bfloat16)
        eq[pl.ds(step * rows, rows), time:] = (gr * vi + gi * vr).astype(jnp.bfloat16)
        return carry

    lax.fori_loop(0, chans, equalize, 0)
    pl.semaphore_wait(barrier, chans - 1 + PLACES)
    own_copy.start()

    def send_eq(step, carry):
        eq_copy(step).start()
        return carry

    lax.fori_loop(1, chans, send_eq, 0)

    def pair_copy(f, p):
        at = f * block + (p * CORES + core) * rows
        return pltpu.make_async_remote_copy(
            samples.at[pl.ds(at, rows)], samples.at[pl.ds(at, rows)], pair_send, pair_recv,
            device_id={"freq": plane * CORES + 1 - core}, device_id_type=MESH)

    def whole(ref, sem):
        return pltpu.make_async_copy(ref, ref, sem)

    row_x, row_z = feed % ROW, feed // ROW

    def near_place(dx, dz):
        return (row_z + dz) % 2 * ROW + (row_x + dx) % ROW

    def pass_on(step, carry):
        dx, dy, dz = offset_of(step)
        p, f = chip_at(plane, feed, 4 - dx, 4 - dy, 4 - dz)
        whole(samples.at[pl.ds(0, rows)], eq_recv.at[f, p]).wait()
        pair_copy(f, p).start()
        return carry

    owner, slot, cols = row_z, row_x, block

    def send(to, col):
        for part in range(2):
            src = tiles.at[to, part, :, pl.ds(pl.multiple_of(col * cols, cols), cols)]
            dst = arrived.at[slot, part, :, pl.ds(pl.multiple_of(core * half + col * cols, cols), cols)]
            far = pltpu.make_async_remote_copy(
                src, dst, out_send, out_recv.at[slot, core * ROW + col],
                device_id={"freq": plane * CORES + owner, "feed": to}, device_id_type=MESH)
            near = pltpu.make_async_copy(src, dst, out_recv.at[slot, core * ROW + col])
            here = jnp.logical_and(to == feed, owner == core)

            @pl.when(here)
            def _():
                near.start()

            @pl.when(jnp.logical_not(here))
            def _():
                far.start()

    def correlate(to, col):
        own = samples[pl.ds(pl.multiple_of(to * block, block), block), :]
        turned = jnp.concatenate([own[:, time:], -own[:, :time]], axis=1)
        left = jnp.concatenate([own, turned], axis=0)
        right = samples[pl.ds(pl.multiple_of(core * half + col * cols, cols), cols), :]
        product = lax.dot_general(left, right, (((1,), (1,)), ((), ())), preferred_element_type=jnp.float32)
        product = (product * (1.0 / time)).astype(jnp.bfloat16)
        at = pl.ds(pl.multiple_of(col * cols, cols), cols)
        tiles[to, 0, :, at] = product[:block]
        tiles[to, 1, :, at] = product[block:]

    def tile_loop(steps, tile):
        def one(step, carry):
            correlate(*tile(step))

            @pl.when(step > 0)
            def _():
                send(*tile(step - 1))
            return carry

        lax.fori_loop(0, steps, one, 0)
        send(*tile(steps - 1))

    far_side = (core + row_z) % 2
    steps = len(TILES[0]) + far_side * (len(TILES[1]) - len(TILES[0]))

    def tile(step):
        close, far = pick(TILES[0], step), pick(TILES[1], step)
        dx, dz, col = (jnp.where(far_side == 1, v, u) for u, v in zip(close, far))
        return near_place(dx, dz), (row_x + col) % ROW

    lax.fori_loop(0, chans, pass_on, 0)
    whole(samples.at[pl.ds(0, half)], pair_recv).wait()
    tile_loop(steps, tile)

    def columns(source, f):
        return arrived.at[source, :, :, pl.ds(pl.multiple_of(f * cols, cols), cols)]

    near_relays = tuple((ax, bx, bz) for (az, ax), (bx, bz) in RELAYS if az == 0)
    far_relays = tuple((ax, bx, bz) for (az, ax), (bx, bz) in RELAYS if az == 1)
    relays = len(near_relays) + far_side * (len(far_relays) - len(near_relays))

    def hand_on(n, carry):
        ax, bx, bz = (jnp.where(far_side == 1, v, u) for u, v in zip(pick(near_relays, n), pick(far_relays, n)))
        source = (row_x - ax + ROW) % ROW
        to = (core + bz) % 2 * ROW + (source + bx) % ROW
        whole(columns(source, to), out_recv.at[source, to]).wait()
        pltpu.make_async_remote_copy(
            columns(source, to), columns(source, feed), relay_send, out_recv.at[source, feed],
            device_id={"freq": plane * CORES + core, "feed": to}, device_id_type=MESH).start()
        return carry

    lax.fori_loop(0, relays, hand_on, 0)

    def landed(i, carry):
        source, f = i // PLACES, i % PLACES
        seen = relayed(far_side, (row_x - source + ROW) % ROW, (f % ROW - source + ROW) % ROW, (f // ROW + core) % 2)

        @pl.when(jnp.logical_not(seen))
        def _():
            whole(columns(source, f), out_recv.at[source, f]).wait()
        return carry

    lax.fori_loop(0, ROW * PLACES, landed, 0)
    whole(eq.at[pl.ds(0, (chans - 1) * rows)], eq_send).wait()
    whole(samples.at[pl.ds(0, half)], pair_send).wait()
    one_tile = tiles.at[0, :, :, pl.ds(0, cols)]

    def sent(i, carry):
        whole(one_tile, out_send).wait()
        return carry

    lax.fori_loop(0, steps - jnp.where(owner == core, ROW, 0), sent, 0)

    def handed(i, carry):
        whole(one_tile, relay_send).wait()
        return carry

    lax.fori_loop(0, relays, handed, 0)


def finish(arrived, out):
    _, core, feed = place()
    source, width = pl.program_id(0), out.shape[2]
    for n in range(out.shape[3] // width):
        f = pl.program_id(1) * (out.shape[3] // width) + n
        turned = relayed((f // ROW + core) % 2, (f % ROW - source + ROW) % ROW,
                         (feed % ROW - source + ROW) % ROW, (feed // ROW + core) % 2)
        at = slice(n * width, (n + 1) * width)
        took = pl.ds(pl.multiple_of(f * width, width), width)

        @pl.when(turned)
        def _():
            out[0, 0, :, at] = arrived[source, 0, :, took].astype(jnp.float32).T
            out[0, 1, :, at] = -arrived[source, 1, :, took].astype(jnp.float32).T

        @pl.when(jnp.logical_not(turned))
        def _():
            out[0, :, :, at] = arrived[source, :, :, took].astype(jnp.float32)


def per_device(voltages, gains):
    chans, rows, _, time = voltages.shape
    feeds = rows * PLANES * CORES * PLACES
    block = feeds // PLACES
    owned = chans // (PLANES * CORES)
    arrived = pl.pallas_call(
        kernel,
        out_shape=pltpu.VMEM((owned, 2, block, feeds), jnp.bfloat16),
        in_specs=[pl.BlockSpec(memory_space=pltpu.HBM), pl.BlockSpec(memory_space=pltpu.VMEM)],
        out_specs=pl.BlockSpec(memory_space=pltpu.VMEM),
        scratch_shapes=[
            pltpu.VMEM((chans, rows, 2, time), jnp.int32),
            pltpu.VMEM((chans * rows, 2 * time), jnp.bfloat16),
            pltpu.VMEM((feeds, 2 * time), jnp.bfloat16),
            pltpu.VMEM((PLACES, 2, block, feeds // CORES), jnp.bfloat16),
            pltpu.SemaphoreType.DMA((chans,)),
            pltpu.SemaphoreType.DMA,
            pltpu.SemaphoreType.DMA((PLACES, PLANES)),
            pltpu.SemaphoreType.DMA,
            pltpu.SemaphoreType.DMA,
            pltpu.SemaphoreType.DMA,
            pltpu.SemaphoreType.DMA((ROW, PLACES)),
            pltpu.SemaphoreType.DMA,
        ],
        compiler_params=pltpu.CompilerParams(collective_id=0, has_side_effects=True, vmem_limit_bytes=45 * 2**20),
        name="x_engine",
    )(voltages, gains.transpose(0, 2, 1))
    spec = pl.BlockSpec((1, 2, block, feeds // 2), lambda i, j: (i, 0, 0, j))
    return pl.pallas_call(
        finish,
        out_shape=jax.ShapeDtypeStruct(arrived.shape, jnp.float32),
        grid=(owned, 2),
        in_specs=[pl.BlockSpec(memory_space=pltpu.VMEM)],
        out_specs=spec,
        compiler_params=pltpu.CompilerParams(vmem_limit_bytes=16 * 2**20),
        name="widen",
    )(arrived)


def solution(mesh):
    in_specs = (P(None, ("feed", "freq"), None, None), P(None, None, ("feed", "freq")))
    out_specs = P("freq", None, "feed", None)
    return jax.shard_map(
        per_device, mesh=mesh, in_specs=in_specs, out_specs=out_specs, check_vma=False
    )
```

```python
import functools

import jax
import jax.numpy as jnp
from jax import lax
from jax.experimental import pallas as pl
from jax.experimental.pallas import tpu as pltpu
from jax.sharding import PartitionSpec as P

MESH = pl.DeviceIdType.MESH
PLANES, PLACES, CORES, ROW = 8, 8, 2, 4


RELAYS = (
    ((0, 3), (2, 1)), ((0, 1), (2, 1)), ((0, 2), (2, 1)), ((0, 1), (1, 1)), ((0, 3), (3, 1)), ((0, 1), (2, 0)), ((0, 3), (2, 0)),
    ((1, 0), (2, 1)), ((1, 1), (2, 1)), ((1, 3), (2, 1)), ((1, 0), (1, 1)), ((1, 0), (3, 1)),
)
TILES = (
    ((1, 0, 2), (3, 0, 2), (0, 1, 0), (1, 1, 0), (3, 1, 0), (2, 0, 0), (1, 0, 0), (3, 0, 0), (0, 1, 1), (1, 1, 2), (3, 1, 1), (2, 1, 0), (1, 0, 1), (3, 0, 1), (0, 1, 2), (2, 0, 2), (1, 1, 3), (3, 1, 2), (1, 0, 3), (3, 0, 3), (0, 1, 3), (0, 0, 0), (0, 0, 1), (0, 0, 2), (0, 0, 3)),
    ((1, 0, 1), (3, 0, 2), (0, 1, 1), (2, 0, 2), (1, 1, 2), (3, 1, 2), (1, 0, 2), (3, 0, 3), (0, 1, 2), (2, 0, 0), (0, 1, 3), (1, 1, 1), (3, 1, 1), (2, 1, 2), (1, 0, 0), (3, 0, 0), (2, 0, 1), (1, 1, 3), (3, 1, 3), (1, 0, 3), (3, 0, 1), (0, 1, 0), (2, 0, 3), (0, 0, 0), (0, 0, 1), (0, 0, 2), (0, 0, 3)),
)


def pick(table, step):
    out = []
    for column in zip(*table):
        value = jnp.int32(column[0])
        for n in range(1, len(column)):
            value = jnp.where(step == n, column[n], value)
        out.append(value)
    return out


def relayed(giver_dz, giver_dx, taker_dx, taker_dz):
    hit = jnp.bool_(False)
    for (az, ax), (bx, bz) in RELAYS:
        same = (giver_dz == az) & (giver_dx == ax) & (taker_dx == bx) & (taker_dz == bz)
        hit = hit | same
    return hit


def place():
    freq, feed = lax.axis_index("freq"), lax.axis_index("feed")
    return freq // 2, freq % 2, feed


def chip_at(plane, feed, dx, dy, dz):
    z = (feed // ROW * 2 + plane % 2 + dz) % 4
    y = (plane // 2 + dy) % 4
    x = (feed % ROW + dx) % 4
    return y * 2 + z % 2, z // 2 * ROW + x


def offset_of(step):
    a, b = step // 4 % 4, step % 4
    return a, b, (step // 16 - a - b + 8) % 4


def kernel(volt, gains, arrived, raw, eq, samples, tiles, raw_sem, eq_send, eq_recv, pair_send, pair_recv, out_send, out_recv, relay_send):
    plane, core, feed = place()
    chans, rows, _, time = volt.shape
    block = rows * PLANES * CORES
    half = block * PLACES // CORES
    me = feed * block + (plane * CORES + core) * rows

    def raw_copy(step):
        p, f = chip_at(plane, feed, *offset_of(step))
        return pltpu.make_async_copy(volt.at[p * PLACES + f], raw.at[step], raw_sem.at[step])

    def start_raw(step, carry):
        raw_copy(step).start()
        return carry


    barrier = pltpu.get_barrier_semaphore()

    def greet(step, carry):
        p, f = chip_at(plane, feed, *offset_of(step))
        pl.semaphore_signal(barrier, inc=1, device_id={"freq": p * CORES + core, "feed": f}, device_id_type=MESH)
        return carry

    def greet_other(f, carry):
        pl.semaphore_signal(barrier, inc=1, device_id={"freq": plane * CORES + 1 - core, "feed": f}, device_id_type=MESH)
        return carry

    lax.fori_loop(1, chans, greet, 0)
    lax.fori_loop(0, PLACES, greet_other, 0)
    lax.fori_loop(0, chans, start_raw, 0)

    def eq_copy(step):
        p, f = chip_at(plane, feed, *offset_of(step))
        return pltpu.make_async_remote_copy(
            eq.at[pl.ds(step * rows, rows)], samples.at[pl.ds(me, rows)], eq_send, eq_recv.at[feed, plane],
            device_id={"freq": p * CORES + core, "feed": f}, device_id_type=MESH)

    own_copy = pltpu.make_async_copy(eq.at[pl.ds(0, rows)], samples.at[pl.ds(me, rows)], eq_recv.at[feed, plane])
    lanes = lax.broadcasted_iota(jnp.int32, (rows, chans), 1)

    def equalize(step, carry):
        raw_copy(step).wait()
        p, f = chip_at(plane, feed, *offset_of(step))
        chan = p * PLACES + f
        gr = jnp.sum(jnp.where(lanes == chan, gains[0], 0.0), axis=1, keepdims=True)
        gi = jnp.sum(jnp.where(lanes == chan, gains[1], 0.0), axis=1, keepdims=True)
        vr = raw[step, :, 0, :].astype(jnp.float32)
        vi = raw[step, :, 1, :].astype(jnp.float32)
        eq[pl.ds(step * rows, rows), :time] = (gr * vr - gi * vi).astype(jnp.bfloat16)
        eq[pl.ds(step * rows, rows), time:] = (gr * vi + gi * vr).astype(jnp.bfloat16)
        return carry

    lax.fori_loop(0, 24, equalize, 0)
    pl.semaphore_wait(barrier, chans - 1 + PLACES)
    own_copy.start()

    def send_eq(step, carry):
        eq_copy(step).start()
        return carry

    lax.fori_loop(1, 24, send_eq, 0)

    def equalize_and_send(step, carry):
        equalize(step, carry)

        @pl.when(step > 24)
        def _():
            eq_copy(step - 1).start()
        return carry

    lax.fori_loop(24, chans, equalize_and_send, 0)
    eq_copy(chans - 1).start()

    def pair_copy(f, p):
        at = f * block + (p * CORES + core) * rows
        return pltpu.make_async_remote_copy(
            samples.at[pl.ds(at, rows)], samples.at[pl.ds(at, rows)], pair_send, pair_recv,
            device_id={"freq": plane * CORES + 1 - core}, device_id_type=MESH)

    def whole(ref, sem):
        return pltpu.make_async_copy(ref, ref, sem)

    row_x, row_z = feed % ROW, feed // ROW

    def near_place(dx, dz):
        return (row_z + dz) % 2 * ROW + (row_x + dx) % ROW

    def pass_on(step, carry):
        dx, dy, dz = offset_of(step)
        p, f = chip_at(plane, feed, 4 - dx, 4 - dy, 4 - dz)
        whole(samples.at[pl.ds(0, rows)], eq_recv.at[f, p]).wait()
        pair_copy(f, p).start()
        return carry

    owner, slot, cols = row_z, row_x, block

    def start(to, col, row, count, lane, width):
        rs = pl.ds(row, count)
        src = tiles.at[to, :, rs, pl.ds(pl.multiple_of(col * cols + lane, width), width)]
        dst = arrived.at[slot, :, rs, pl.ds(pl.multiple_of(core * half + col * cols + lane, width), width)]
        landing = out_recv.at[slot, core * ROW + col]
        far = pltpu.make_async_remote_copy(
            src, dst, out_send, landing, device_id={"freq": plane * CORES + owner, "feed": to}, device_id_type=MESH)
        near = pltpu.make_async_copy(src, dst, landing)
        here = jnp.logical_and(to == feed, owner == core)

        @pl.when(here)
        def _():
            near.start()

        @pl.when(jnp.logical_not(here))
        def _():
            far.start()

    def send(to, col):
        diagonal = to == core * ROW + col

        @pl.when(diagonal)
        def _():
            start(to, col, 0, cols // 2, 0, cols)
            start(to, col, cols // 2, cols // 2, cols // 2, cols // 2)

        @pl.when(jnp.logical_not(diagonal))
        def _():
            start(to, col, 0, cols, 0, cols)

    def correlate(to, col):
        own = samples[pl.ds(pl.multiple_of(to * block, block), block), :]
        turned = jnp.concatenate([own[:, time:], -own[:, :time]], axis=1)
        left = jnp.concatenate([own, turned], axis=0)
        right = samples[pl.ds(pl.multiple_of(core * half + col * cols, cols), cols), :]
        product = lax.dot_general(left, right, (((1,), (1,)), ((), ())), preferred_element_type=jnp.float32)
        product = (product * (1.0 / time)).astype(jnp.bfloat16)
        at = pl.ds(pl.multiple_of(col * cols, cols), cols)
        tiles[to, 0, :, at] = product[:block]
        tiles[to, 1, :, at] = product[block:]

    def tile_loop(steps, tile):
        def one(step, carry):
            correlate(*tile(step))

            @pl.when(step > 0)
            def _():
                send(*tile(step - 1))
            return carry

        lax.fori_loop(0, steps, one, 0)
        send(*tile(steps - 1))

    far_side = (core + row_z) % 2
    steps = len(TILES[0]) + far_side * (len(TILES[1]) - len(TILES[0]))

    def tile(step):
        close, far = pick(TILES[0], step), pick(TILES[1], step)
        dx, dz, col = (jnp.where(far_side == 1, v, u) for u, v in zip(close, far))
        return near_place(dx, dz), (row_x + col) % ROW

    lax.fori_loop(0, chans, pass_on, 0)
    whole(samples.at[pl.ds(0, half)], pair_recv).wait()
    tile_loop(steps, tile)

    def columns(source, f):
        return arrived.at[source, :, :, pl.ds(pl.multiple_of(f * cols, cols), cols)]

    near_relays = tuple((ax, bx, bz) for (az, ax), (bx, bz) in RELAYS if az == 0)
    far_relays = tuple((ax, bx, bz) for (az, ax), (bx, bz) in RELAYS if az == 1)
    relays = len(near_relays) + far_side * (len(far_relays) - len(near_relays))

    def hand_on(n, carry):
        ax, bx, bz = (jnp.where(far_side == 1, v, u) for u, v in zip(pick(near_relays, n), pick(far_relays, n)))
        source = (row_x - ax + ROW) % ROW
        to = (core + bz) % 2 * ROW + (source + bx) % ROW
        whole(columns(source, to), out_recv.at[source, to]).wait()
        pltpu.make_async_remote_copy(
            columns(source, to), columns(source, feed), relay_send, out_recv.at[source, feed],
            device_id={"freq": plane * CORES + core, "feed": to}, device_id_type=MESH).start()
        return carry

    lax.fori_loop(0, relays, hand_on, 0)

    def landed(i, carry):
        source, f = i // PLACES, i % PLACES
        seen = relayed(far_side, (row_x - source + ROW) % ROW, (f % ROW - source + ROW) % ROW, (f // ROW + core) % 2)

        @pl.when(jnp.logical_not(seen | (f == feed)))
        def _():
            whole(columns(source, f), out_recv.at[source, f]).wait()

        @pl.when(f == feed)
        def _():
            whole(tiles.at[0, :, pl.ds(0, cols - cols // 4), pl.ds(0, cols)], out_recv.at[source, f]).wait()
        return carry

    lax.fori_loop(0, ROW * PLACES, landed, 0)
    whole(eq.at[pl.ds(0, (chans - 1) * rows)], eq_send).wait()
    whole(samples.at[pl.ds(0, half)], pair_send).wait()
    one_tile = tiles.at[0, :, :, pl.ds(0, cols)]

    def sent(i, carry):
        whole(one_tile, out_send).wait()
        return carry

    quarters = 4 * steps - jnp.where(owner == core, 4 * ROW + ROW - 1, ROW)
    lax.fori_loop(0, quarters // 4, sent, 0)

    def sent_quarter(i, carry):
        whole(tiles.at[0, :, pl.ds(0, cols // 4), pl.ds(0, cols)], out_send).wait()
        return carry

    lax.fori_loop(0, quarters % 4, sent_quarter, 0)

    def handed(i, carry):
        whole(one_tile, relay_send).wait()
        return carry

    lax.fori_loop(0, relays, handed, 0)


def finish(arrived, out):
    _, core, feed = place()
    source, width = pl.program_id(0), out.shape[2]
    for n in range(out.shape[3] // width):
        f = pl.program_id(1) * (out.shape[3] // width) + n
        turned = relayed((f // ROW + core) % 2, (f % ROW - source + ROW) % ROW,
                         (feed % ROW - source + ROW) % ROW, (feed // ROW + core) % 2)
        at = slice(n * width, (n + 1) * width)
        took = pl.ds(pl.multiple_of(f * width, width), width)

        re, im = (arrived[source, part, :, took].astype(jnp.float32) for part in range(2))

        @pl.when(turned)
        def _():
            out[0, 0, :, at] = re.T
            out[0, 1, :, at] = -im.T

        @pl.when(jnp.logical_not(turned))
        def _():
            out[0, 0, :, at] = re
            out[0, 1, :, at] = im

        @pl.when(f == feed)
        def _():
            low, cut = slice(n * width, n * width + width // 2), width // 2
            out[0, 0, cut:, low] = re[:cut, cut:].T
            out[0, 1, cut:, low] = -im[:cut, cut:].T


def per_device(voltages, gains):
    chans, rows, _, time = voltages.shape
    feeds = rows * PLANES * CORES * PLACES
    block = feeds // PLACES
    owned = chans // (PLANES * CORES)
    arrived = pl.pallas_call(
        kernel,
        out_shape=pltpu.VMEM((owned, 2, block, feeds), jnp.bfloat16),
        in_specs=[pl.BlockSpec(memory_space=pltpu.HBM), pl.BlockSpec(memory_space=pltpu.VMEM)],
        out_specs=pl.BlockSpec(memory_space=pltpu.VMEM),
        scratch_shapes=[
            pltpu.VMEM((chans, rows, 2, time), jnp.int32),
            pltpu.VMEM((chans * rows, 2 * time), jnp.bfloat16),
            pltpu.VMEM((feeds, 2 * time), jnp.bfloat16),
            pltpu.VMEM((PLACES, 2, block, feeds // CORES), jnp.bfloat16),
            pltpu.SemaphoreType.DMA((chans,)),
            pltpu.SemaphoreType.DMA,
            pltpu.SemaphoreType.DMA((PLACES, PLANES)),
            pltpu.SemaphoreType.DMA,
            pltpu.SemaphoreType.DMA,
            pltpu.SemaphoreType.DMA,
            pltpu.SemaphoreType.DMA((ROW, PLACES)),
            pltpu.SemaphoreType.DMA,
        ],
        compiler_params=pltpu.CompilerParams(collective_id=0, has_side_effects=True, vmem_limit_bytes=45 * 2**20),
        name="x_engine",
    )(voltages, gains.transpose(0, 2, 1))
    spec = pl.BlockSpec((1, 2, block, feeds // 2), lambda i, j: (i, 0, 0, j))
    return pl.pallas_call(
        finish,
        out_shape=jax.ShapeDtypeStruct(arrived.shape, jnp.float32),
        grid=(owned, 2),
        in_specs=[pl.BlockSpec(memory_space=pltpu.VMEM)],
        out_specs=spec,
        compiler_params=pltpu.CompilerParams(vmem_limit_bytes=16 * 2**20),
        name="widen",
    )(arrived)


def solution(mesh):
    in_specs = (P(None, ("feed", "freq"), None, None), P(None, None, ("feed", "freq")))
    out_specs = P("freq", None, "feed", None)
    return jax.shard_map(
        per_device, mesh=mesh, in_specs=in_specs, out_specs=out_specs, check_vma=False
    )
```

```python
import functools

import jax
import jax.numpy as jnp
from jax import lax
from jax.experimental import pallas as pl
from jax.experimental.pallas import tpu as pltpu
from jax.sharding import PartitionSpec as P

MESH = pl.DeviceIdType.MESH
PLANES, PLACES, CORES, ROW = 8, 8, 2, 4


RELAYS = (
    ((0, 3), (2, 1)), ((0, 1), (2, 1)), ((0, 2), (2, 1)), ((0, 1), (1, 1)), ((0, 3), (3, 1)), ((0, 1), (2, 0)), ((0, 3), (2, 0)),
    ((1, 0), (2, 1)), ((1, 1), (2, 1)), ((1, 3), (2, 1)), ((1, 0), (1, 1)), ((1, 0), (3, 1)),
)
TILES = (
    ((1, 0, 2), (3, 0, 2), (0, 1, 0), (1, 1, 0), (3, 1, 0), (2, 0, 0), (0, 1, 1), (1, 0, 0), (3, 0, 0), (1, 1, 2), (3, 1, 1), (2, 1, 0), (0, 1, 2), (1, 0, 1), (3, 0, 1), (2, 0, 2), (1, 1, 3), (3, 1, 2), (0, 1, 3), (1, 0, 3), (3, 0, 3), (0, 0, 0), (0, 0, 1), (0, 0, 2), (0, 0, 3)),
    ((0, 1, 1), (1, 0, 1), (3, 0, 2), (2, 0, 2), (1, 1, 2), (3, 1, 2), (0, 1, 2), (1, 0, 2), (3, 0, 3), (2, 0, 0), (0, 1, 3), (1, 1, 1), (3, 1, 1), (2, 1, 2), (1, 0, 0), (3, 0, 0), (2, 0, 1), (1, 1, 3), (3, 1, 3), (0, 1, 0), (1, 0, 3), (3, 0, 1), (2, 0, 3), (0, 0, 0), (0, 0, 1), (0, 0, 2), (0, 0, 3)),
)


def pick(table, step):
    out = []
    for column in zip(*table):
        value = jnp.int32(column[0])
        for n in range(1, len(column)):
            value = jnp.where(step == n, column[n], value)
        out.append(value)
    return out


def relayed(giver_dz, giver_dx, taker_dx, taker_dz):
    hit = jnp.bool_(False)
    for (az, ax), (bx, bz) in RELAYS:
        same = (giver_dz == az) & (giver_dx == ax) & (taker_dx == bx) & (taker_dz == bz)
        hit = hit | same
    return hit


def place():
    freq, feed = lax.axis_index("freq"), lax.axis_index("feed")
    return freq // 2, freq % 2, feed


def chip_at(plane, feed, dx, dy, dz):
    z = (feed // ROW * 2 + plane % 2 + dz) % 4
    y = (plane // 2 + dy) % 4
    x = (feed % ROW + dx) % 4
    return y * 2 + z % 2, z // 2 * ROW + x


def offset_of(step):
    a, b = step % 4, step // 4 % 4
    return a, (a + step // 16) % 4, (a * 3 + b) % 4


def kernel(volt, gains, arrived, raw, eq, samples, tiles, raw_sem, eq_send, eq_recv, pair_send, pair_recv, out_send, out_recv, relay_send):
    plane, core, feed = place()
    chans, rows, _, time = volt.shape
    block = rows * PLANES * CORES
    half = block * PLACES // CORES
    me = feed * block + (plane * CORES + core) * rows

    def raw_copy(step):
        p, f = chip_at(plane, feed, *offset_of(step))
        return pltpu.make_async_copy(volt.at[p * PLACES + f], raw.at[step], raw_sem.at[step])

    def start_raw(step, carry):
        raw_copy(step).start()
        return carry


    barrier = pltpu.get_barrier_semaphore()

    def greet(step, carry):
        p, f = chip_at(plane, feed, *offset_of(step))
        pl.semaphore_signal(barrier, inc=1, device_id={"freq": p * CORES + core, "feed": f}, device_id_type=MESH)
        return carry

    def greet_other(f, carry):
        pl.semaphore_signal(barrier, inc=1, device_id={"freq": plane * CORES + 1 - core, "feed": f}, device_id_type=MESH)
        return carry

    lax.fori_loop(1, chans, greet, 0)
    lax.fori_loop(0, PLACES, greet_other, 0)
    lax.fori_loop(0, chans, start_raw, 0)

    def eq_copy(step):
        p, f = chip_at(plane, feed, *offset_of(step))
        return pltpu.make_async_remote_copy(
            eq.at[pl.ds(step * rows, rows)], samples.at[pl.ds(me, rows)], eq_send, eq_recv.at[feed, plane],
            device_id={"freq": p * CORES + core, "feed": f}, device_id_type=MESH)

    own_copy = pltpu.make_async_copy(eq.at[pl.ds(0, rows)], samples.at[pl.ds(me, rows)], eq_recv.at[feed, plane])
    lanes = lax.broadcasted_iota(jnp.int32, (rows, chans), 1)

    def equalize(step, carry):
        raw_copy(step).wait()
        p, f = chip_at(plane, feed, *offset_of(step))
        chan = p * PLACES + f
        gr = jnp.sum(jnp.where(lanes == chan, gains[0], 0.0), axis=1, keepdims=True)
        gi = jnp.sum(jnp.where(lanes == chan, gains[1], 0.0), axis=1, keepdims=True)
        vr = raw[step, :, 0, :].astype(jnp.float32)
        vi = raw[step, :, 1, :].astype(jnp.float32)
        eq[pl.ds(step * rows, rows), :time] = (gr * vr - gi * vi).astype(jnp.bfloat16)
        eq[pl.ds(step * rows, rows), time:] = (gr * vi + gi * vr).astype(jnp.bfloat16)
        return carry

    lax.fori_loop(0, 24, equalize, 0)
    pl.semaphore_wait(barrier, chans - 1 + PLACES)
    own_copy.start()

    def send_eq(step, carry):
        eq_copy(step).start()
        return carry

    lax.fori_loop(1, 24, send_eq, 0)

    def equalize_and_send(step, carry):
        equalize(step, carry)

        @pl.when(step > 24)
        def _():
            eq_copy(step - 1).start()
        return carry

    lax.fori_loop(24, chans, equalize_and_send, 0)
    eq_copy(chans - 1).start()

    def pair_copy(f, p):
        at = f * block + (p * CORES + core) * rows
        return pltpu.make_async_remote_copy(
            samples.at[pl.ds(at, rows)], samples.at[pl.ds(at, rows)], pair_send, pair_recv,
            device_id={"freq": plane * CORES + 1 - core}, device_id_type=MESH)

    def whole(ref, sem):
        return pltpu.make_async_copy(ref, ref, sem)

    row_x, row_z = feed % ROW, feed // ROW

    def near_place(dx, dz):
        return (row_z + dz) % 2 * ROW + (row_x + dx) % ROW

    def pass_on(step, carry):
        dx, dy, dz = offset_of(step)
        p, f = chip_at(plane, feed, 4 - dx, 4 - dy, 4 - dz)
        whole(samples.at[pl.ds(0, rows)], eq_recv.at[f, p]).wait()
        pair_copy(f, p).start()
        return carry

    owner, slot, cols = row_z, row_x, block

    def start(to, col, row, count, lane, width):
        rs = pl.ds(row, count)
        src = tiles.at[to, :, rs, pl.ds(pl.multiple_of(col * cols + lane, width), width)]
        dst = arrived.at[slot, :, rs, pl.ds(pl.multiple_of(core * half + col * cols + lane, width), width)]
        landing = out_recv.at[slot, core * ROW + col]
        far = pltpu.make_async_remote_copy(
            src, dst, out_send, landing, device_id={"freq": plane * CORES + owner, "feed": to}, device_id_type=MESH)
        near = pltpu.make_async_copy(src, dst, landing)
        here = jnp.logical_and(to == feed, owner == core)

        @pl.when(here)
        def _():
            near.start()

        @pl.when(jnp.logical_not(here))
        def _():
            far.start()

    def send(to, col):
        diagonal = to == core * ROW + col

        @pl.when(diagonal)
        def _():
            start(to, col, 0, cols // 2, 0, cols)
            start(to, col, cols // 2, cols // 2, cols // 2, cols // 2)

        @pl.when(jnp.logical_not(diagonal))
        def _():
            start(to, col, 0, cols, 0, cols)

    def correlate(to, col):
        own = samples[pl.ds(pl.multiple_of(to * block, block), block), :]
        turned = jnp.concatenate([own[:, time:], -own[:, :time]], axis=1)
        left = jnp.concatenate([own, turned], axis=0)
        right = samples[pl.ds(pl.multiple_of(core * half + col * cols, cols), cols), :]
        product = lax.dot_general(left, right, (((1,), (1,)), ((), ())), preferred_element_type=jnp.float32)
        product = (product * (1.0 / time)).astype(jnp.bfloat16)
        at = pl.ds(pl.multiple_of(col * cols, cols), cols)
        tiles[to, 0, :, at] = product[:block]
        tiles[to, 1, :, at] = product[block:]

    def tile_loop(steps, tile):
        def one(step, carry):
            correlate(*tile(step))

            @pl.when(step > 0)
            def _():
                send(*tile(step - 1))
            return carry

        lax.fori_loop(0, steps, one, 0)
        send(*tile(steps - 1))

    far_side = (core + row_z) % 2
    steps = len(TILES[0]) + far_side * (len(TILES[1]) - len(TILES[0]))

    def tile(step):
        close, far = pick(TILES[0], step), pick(TILES[1], step)
        dx, dz, col = (jnp.where(far_side == 1, v, u) for u, v in zip(close, far))
        return near_place(dx, dz), (row_x + col) % ROW

    lax.fori_loop(0, chans, pass_on, 0)
    whole(samples.at[pl.ds(0, half)], pair_recv).wait()
    tile_loop(steps, tile)

    def columns(source, f):
        return arrived.at[source, :, :, pl.ds(pl.multiple_of(f * cols, cols), cols)]

    near_relays = tuple((ax, bx, bz) for (az, ax), (bx, bz) in RELAYS if az == 0)
    far_relays = tuple((ax, bx, bz) for (az, ax), (bx, bz) in RELAYS if az == 1)
    relays = len(near_relays) + far_side * (len(far_relays) - len(near_relays))

    def hand_on(n, carry):
        ax, bx, bz = (jnp.where(far_side == 1, v, u) for u, v in zip(pick(near_relays, n), pick(far_relays, n)))
        source = (row_x - ax + ROW) % ROW
        to = (core + bz) % 2 * ROW + (source + bx) % ROW
        whole(columns(source, to), out_recv.at[source, to]).wait()
        for part in range(4):
            rs = pl.ds(part * (cols // 4), cols // 4)
            pltpu.make_async_remote_copy(
                arrived.at[source, :, rs, pl.ds(pl.multiple_of(to * cols, cols), cols)],
                arrived.at[source, :, rs, pl.ds(pl.multiple_of(feed * cols, cols), cols)], relay_send, out_recv.at[source, feed],
                device_id={"freq": plane * CORES + core, "feed": to}, device_id_type=MESH).start()
        return carry

    lax.fori_loop(0, relays, hand_on, 0)

    def landed(i, carry):
        source, f = i // PLACES, i % PLACES
        seen = relayed(far_side, (row_x - source + ROW) % ROW, (f % ROW - source + ROW) % ROW, (f // ROW + core) % 2)

        @pl.when(jnp.logical_not(seen | (f == feed)))
        def _():
            whole(columns(source, f), out_recv.at[source, f]).wait()

        @pl.when(f == feed)
        def _():
            whole(tiles.at[0, :, pl.ds(0, cols - cols // 4), pl.ds(0, cols)], out_recv.at[source, f]).wait()
        return carry

    lax.fori_loop(0, ROW * PLACES, landed, 0)
    whole(eq.at[pl.ds(0, (chans - 1) * rows)], eq_send).wait()
    whole(samples.at[pl.ds(0, half)], pair_send).wait()
    one_tile = tiles.at[0, :, :, pl.ds(0, cols)]

    def sent(i, carry):
        whole(one_tile, out_send).wait()
        return carry

    quarters = 4 * steps - jnp.where(owner == core, 4 * ROW + ROW - 1, ROW)
    lax.fori_loop(0, quarters // 4, sent, 0)

    def sent_quarter(i, carry):
        whole(tiles.at[0, :, pl.ds(0, cols // 4), pl.ds(0, cols)], out_send).wait()
        return carry

    lax.fori_loop(0, quarters % 4, sent_quarter, 0)

    def handed(i, carry):
        whole(one_tile, relay_send).wait()
        return carry

    lax.fori_loop(0, relays, handed, 0)


def finish(arrived, out):
    _, core, feed = place()
    source, width = pl.program_id(0), out.shape[2]
    for n in range(out.shape[3] // width):
        f = n
        turned = relayed((f // ROW + core) % 2, (f % ROW - source + ROW) % ROW,
                         (feed % ROW - source + ROW) % ROW, (feed // ROW + core) % 2)
        at = slice(n * width, (n + 1) * width)
        took = at

        re, im = (arrived[source, part, :, took].astype(jnp.float32) for part in range(2))

        @pl.when(turned)
        def _():
            out[0, 0, :, at] = re.T
            out[0, 1, :, at] = -im.T

        @pl.when(jnp.logical_not(turned))
        def _():
            out[0, 0, :, at] = re
            out[0, 1, :, at] = im

        @pl.when(f == feed)
        def _():
            low, cut = slice(n * width, n * width + width // 2), width // 2
            out[0, 0, cut:, low] = re[:cut, cut:].T
            out[0, 1, cut:, low] = -im[:cut, cut:].T


def per_device(voltages, gains):
    chans, rows, _, time = voltages.shape
    feeds = rows * PLANES * CORES * PLACES
    block = feeds // PLACES
    owned = chans // (PLANES * CORES)
    arrived = pl.pallas_call(
        kernel,
        out_shape=pltpu.VMEM((owned, 2, block, feeds), jnp.bfloat16),
        in_specs=[pl.BlockSpec(memory_space=pltpu.HBM), pl.BlockSpec(memory_space=pltpu.VMEM)],
        out_specs=pl.BlockSpec(memory_space=pltpu.VMEM),
        scratch_shapes=[
            pltpu.VMEM((chans, rows, 2, time), jnp.int32),
            pltpu.VMEM((chans * rows, 2 * time), jnp.bfloat16),
            pltpu.VMEM((feeds, 2 * time), jnp.bfloat16),
            pltpu.VMEM((PLACES, 2, block, feeds // CORES), jnp.bfloat16),
            pltpu.SemaphoreType.DMA((chans,)),
            pltpu.SemaphoreType.DMA,
            pltpu.SemaphoreType.DMA((PLACES, PLANES)),
            pltpu.SemaphoreType.DMA,
            pltpu.SemaphoreType.DMA,
            pltpu.SemaphoreType.DMA,
            pltpu.SemaphoreType.DMA((ROW, PLACES)),
            pltpu.SemaphoreType.DMA,
        ],
        compiler_params=pltpu.CompilerParams(collective_id=0, has_side_effects=True, vmem_limit_bytes=45 * 2**20),
        name="x_engine",
    )(voltages, gains.transpose(0, 2, 1))
    spec = pl.BlockSpec((1, 2, block, feeds), lambda i: (i, 0, 0, 0))
    return pl.pallas_call(
        finish,
        out_shape=jax.ShapeDtypeStruct(arrived.shape, jnp.float32),
        grid=(owned,),
        in_specs=[pl.BlockSpec(memory_space=pltpu.VMEM)],
        out_specs=spec,
        compiler_params=pltpu.CompilerParams(vmem_limit_bytes=24 * 2**20),
        name="widen",
    )(arrived)


def solution(mesh):
    in_specs = (P(None, ("feed", "freq"), None, None), P(None, None, ("feed", "freq")))
    out_specs = P("freq", None, "feed", None)
    return jax.shard_map(
        per_device, mesh=mesh, in_specs=in_specs, out_specs=out_specs, check_vma=False
    )
```

```python
import functools

import jax
import jax.numpy as jnp
from jax import lax
from jax.experimental import pallas as pl
from jax.experimental.pallas import tpu as pltpu
from jax.sharding import PartitionSpec as P

MESH = pl.DeviceIdType.MESH
PLANES, PLACES, CORES, ROW = 8, 8, 2, 4


RELAYS = (
    ((0, 3), (2, 1)), ((0, 1), (2, 1)), ((0, 2), (2, 1)), ((0, 1), (1, 1)), ((0, 3), (3, 1)), ((0, 1), (2, 0)), ((0, 3), (2, 0)),
    ((1, 0), (2, 1)), ((1, 1), (2, 1)), ((1, 3), (2, 1)), ((1, 0), (1, 1)), ((1, 0), (3, 1)),
)
TILES = (
    ((1, 0, 2), (3, 0, 2), (0, 1, 0), (1, 1, 0), (3, 1, 0), (2, 0, 0), (0, 1, 1), (1, 0, 0), (3, 0, 0), (1, 1, 2), (3, 1, 1), (2, 1, 0), (0, 1, 2), (1, 0, 1), (3, 0, 1), (2, 0, 2), (1, 1, 3), (3, 1, 2), (0, 1, 3), (1, 0, 3), (3, 0, 3), (0, 0, 0), (0, 0, 1), (0, 0, 2), (0, 0, 3)),
    ((0, 1, 1), (1, 0, 1), (3, 0, 2), (2, 0, 2), (1, 1, 2), (3, 1, 2), (0, 1, 2), (1, 0, 2), (3, 0, 3), (2, 0, 0), (0, 1, 3), (1, 1, 1), (3, 1, 1), (2, 1, 2), (1, 0, 0), (3, 0, 0), (2, 0, 1), (1, 1, 3), (3, 1, 3), (0, 1, 0), (1, 0, 3), (3, 0, 1), (2, 0, 3), (0, 0, 0), (0, 0, 1), (0, 0, 2), (0, 0, 3)),
)


def pick(table, step):
    out = []
    for column in zip(*table):
        value = jnp.int32(column[0])
        for n in range(1, len(column)):
            value = jnp.where(step == n, column[n], value)
        out.append(value)
    return out


def relayed(giver_dz, giver_dx, taker_dx, taker_dz):
    hit = jnp.bool_(False)
    for (az, ax), (bx, bz) in RELAYS:
        same = (giver_dz == az) & (giver_dx == ax) & (taker_dx == bx) & (taker_dz == bz)
        hit = hit | same
    return hit


def place():
    freq, feed = lax.axis_index("freq"), lax.axis_index("feed")
    return freq // 2, freq % 2, feed


def chip_at(plane, feed, dx, dy, dz):
    z = (feed // ROW * 2 + plane % 2 + dz) % 4
    y = (plane // 2 + dy) % 4
    x = (feed % ROW + dx) % 4
    return y * 2 + z % 2, z // 2 * ROW + x


def offset_of(step):
    a, b = step % 4, step // 4 % 4
    return a, (a + step // 16) % 4, (a * 3 + b) % 4


def kernel(volt, gains, arrived, raw, eq, samples, tiles, raw_sem, eq_send, eq_recv, pair_send, pair_recv, out_send, out_recv, relay_send):
    plane, core, feed = place()
    chans, rows, _, time = volt.shape
    block = rows * PLANES * CORES
    half = block * PLACES // CORES
    me = feed * block + (plane * CORES + core) * rows

    def raw_copy(step):
        p, f = chip_at(plane, feed, *offset_of(step))
        return pltpu.make_async_copy(volt.at[p * PLACES + f], raw.at[step], raw_sem.at[step])

    def start_raw(step, carry):
        raw_copy(step).start()
        return carry


    barrier = pltpu.get_barrier_semaphore()

    def greet(step, carry):
        p, f = chip_at(plane, feed, *offset_of(step))
        pl.semaphore_signal(barrier, inc=1, device_id={"freq": p * CORES + core, "feed": f}, device_id_type=MESH)
        return carry

    def greet_other(f, carry):
        pl.semaphore_signal(barrier, inc=1, device_id={"freq": plane * CORES + 1 - core, "feed": f}, device_id_type=MESH)
        return carry

    lax.fori_loop(1, chans, greet, 0)
    lax.fori_loop(0, PLACES, greet_other, 0)
    lax.fori_loop(0, chans, start_raw, 0)

    def eq_copy(step):
        p, f = chip_at(plane, feed, *offset_of(step))
        return pltpu.make_async_remote_copy(
            eq.at[pl.ds(step * rows, rows)], samples.at[pl.ds(me, rows)], eq_send, eq_recv.at[feed, plane],
            device_id={"freq": p * CORES + core, "feed": f}, device_id_type=MESH)

    own_copy = pltpu.make_async_copy(eq.at[pl.ds(0, rows)], samples.at[pl.ds(me, rows)], eq_recv.at[feed, plane])
    lanes = lax.broadcasted_iota(jnp.int32, (rows, chans), 1)

    def equalize(step, carry):
        raw_copy(step).wait()
        p, f = chip_at(plane, feed, *offset_of(step))
        chan = p * PLACES + f
        gr = jnp.sum(jnp.where(lanes == chan, gains[0], 0.0), axis=1, keepdims=True)
        gi = jnp.sum(jnp.where(lanes == chan, gains[1], 0.0), axis=1, keepdims=True)
        vr = raw[step, :, 0, :].astype(jnp.float32)
        vi = raw[step, :, 1, :].astype(jnp.float32)
        eq[pl.ds(step * rows, rows), :time] = (gr * vr - gi * vi).astype(jnp.bfloat16)
        eq[pl.ds(step * rows, rows), time:] = (gr * vi + gi * vr).astype(jnp.bfloat16)
        return carry

    lax.fori_loop(0, 16, equalize, 0)
    pl.semaphore_wait(barrier, chans - 1 + PLACES)
    own_copy.start()

    def send_eq(step, carry):
        eq_copy(step).start()
        return carry

    lax.fori_loop(1, 16, send_eq, 0)

    def equalize_and_send(step, carry):
        equalize(step, carry)

        @pl.when(step > 16)
        def _():
            eq_copy(step - 1).start()
        return carry

    lax.fori_loop(16, chans, equalize_and_send, 0)

    def pair_copy(f, p):
        at = f * block + (p * CORES + core) * rows
        return pltpu.make_async_remote_copy(
            samples.at[pl.ds(at, rows)], samples.at[pl.ds(at, rows)], pair_send, pair_recv,
            device_id={"freq": plane * CORES + 1 - core}, device_id_type=MESH)

    def whole(ref, sem):
        return pltpu.make_async_copy(ref, ref, sem)

    row_x, row_z = feed % ROW, feed // ROW

    def near_place(dx, dz):
        return (row_z + dz) % 2 * ROW + (row_x + dx) % ROW

    def pass_on(step, carry):
        dx, dy, dz = offset_of(step)
        p, f = chip_at(plane, feed, 4 - dx, 4 - dy, 4 - dz)
        whole(samples.at[pl.ds(0, rows)], eq_recv.at[f, p]).wait()
        pair_copy(f, p).start()
        return carry

    owner, slot, cols = row_z, row_x, block

    def start(to, col, row, count, lane, width):
        rs = pl.ds(row, count)
        src = tiles.at[to, :, rs, pl.ds(pl.multiple_of(col * cols + lane, width), width)]
        dst = arrived.at[slot, :, rs, pl.ds(pl.multiple_of(core * half + col * cols + lane, width), width)]
        landing = out_recv.at[slot, core * ROW + col]
        far = pltpu.make_async_remote_copy(
            src, dst, out_send, landing, device_id={"freq": plane * CORES + owner, "feed": to}, device_id_type=MESH)
        near = pltpu.make_async_copy(src, dst, landing)
        here = jnp.logical_and(to == feed, owner == core)

        @pl.when(here)
        def _():
            near.start()

        @pl.when(jnp.logical_not(here))
        def _():
            far.start()

    def send(to, col):
        diagonal = to == core * ROW + col

        @pl.when(diagonal)
        def _():
            start(to, col, 0, cols // 2, 0, cols)
            start(to, col, cols // 2, cols // 2, cols // 2, cols // 2)

        @pl.when(jnp.logical_not(diagonal))
        def _():
            start(to, col, 0, cols, 0, cols)

    def correlate(to, col):
        own = samples[pl.ds(pl.multiple_of(to * block, block), block), :]
        turned = jnp.concatenate([own[:, time:], -own[:, :time]], axis=1)
        left = jnp.concatenate([own, turned], axis=0)
        right = samples[pl.ds(pl.multiple_of(core * half + col * cols, cols), cols), :]
        product = lax.dot_general(left, right, (((1,), (1,)), ((), ())), preferred_element_type=jnp.float32)
        product = (product * (1.0 / time)).astype(jnp.bfloat16)
        at = pl.ds(pl.multiple_of(col * cols, cols), cols)
        tiles[to, 0, :, at] = product[:block]
        tiles[to, 1, :, at] = product[block:]

    def tile_loop(steps, tile):
        def one(step, carry):
            correlate(*tile(step))

            @pl.when(step > 0)
            def _():
                send(*tile(step - 1))
            return carry

        lax.fori_loop(0, steps, one, 0)

    far_side = (core + row_z) % 2
    steps = len(TILES[0]) + far_side * (len(TILES[1]) - len(TILES[0]))

    def tile(step):
        close, far = pick(TILES[0], step), pick(TILES[1], step)
        dx, dz, col = (jnp.where(far_side == 1, v, u) for u, v in zip(close, far))
        return near_place(dx, dz), (row_x + col) % ROW

    pass_on(0, 0)
    eq_copy(chans - 1).start()
    lax.fori_loop(1, chans, pass_on, 0)
    whole(samples.at[pl.ds(0, half)], pair_recv).wait()
    tile_loop(steps, tile)

    def columns(source, f):
        return arrived.at[source, :, :, pl.ds(pl.multiple_of(f * cols, cols), cols)]

    near_relays = tuple((ax, bx, bz) for (az, ax), (bx, bz) in RELAYS if az == 0)
    far_relays = tuple((ax, bx, bz) for (az, ax), (bx, bz) in RELAYS if az == 1)
    relays = len(near_relays) + far_side * (len(far_relays) - len(near_relays))

    def hand_on(n, carry):
        ax, bx, bz = (jnp.where(far_side == 1, v, u) for u, v in zip(pick(near_relays, n), pick(far_relays, n)))
        source = (row_x - ax + ROW) % ROW
        to = (core + bz) % 2 * ROW + (source + bx) % ROW
        whole(columns(source, to), out_recv.at[source, to]).wait()
        for part in range(4):
            rs = pl.ds(part * (cols // 4), cols // 4)
            pltpu.make_async_remote_copy(
                arrived.at[source, :, rs, pl.ds(pl.multiple_of(to * cols, cols), cols)],
                arrived.at[source, :, rs, pl.ds(pl.multiple_of(feed * cols, cols), cols)], relay_send, out_recv.at[source, feed],
                device_id={"freq": plane * CORES + core, "feed": to}, device_id_type=MESH).start()
        return carry

    lax.fori_loop(0, relays, hand_on, 0)
    send(*tile(steps - 1))

    def landed(i, carry):
        source, f = i // PLACES, i % PLACES
        seen = relayed(far_side, (row_x - source + ROW) % ROW, (f % ROW - source + ROW) % ROW, (f // ROW + core) % 2)

        @pl.when(jnp.logical_not(seen | (f == feed)))
        def _():
            whole(columns(source, f), out_recv.at[source, f]).wait()

        @pl.when(f == feed)
        def _():
            whole(tiles.at[0, :, pl.ds(0, cols - cols // 4), pl.ds(0, cols)], out_recv.at[source, f]).wait()
        return carry

    lax.fori_loop(0, ROW * PLACES, landed, 0)
    whole(eq.at[pl.ds(0, (chans - 1) * rows)], eq_send).wait()
    whole(samples.at[pl.ds(0, half)], pair_send).wait()
    one_tile = tiles.at[0, :, :, pl.ds(0, cols)]

    def sent(i, carry):
        whole(one_tile, out_send).wait()
        return carry

    quarters = 4 * steps - jnp.where(owner == core, 4 * ROW + ROW - 1, ROW)
    lax.fori_loop(0, quarters // 4, sent, 0)

    def sent_quarter(i, carry):
        whole(tiles.at[0, :, pl.ds(0, cols // 4), pl.ds(0, cols)], out_send).wait()
        return carry

    lax.fori_loop(0, quarters % 4, sent_quarter, 0)

    def handed(i, carry):
        whole(one_tile, relay_send).wait()
        return carry

    lax.fori_loop(0, relays, handed, 0)


def finish(arrived, out):
    _, core, feed = place()
    source, width = pl.program_id(0), out.shape[2]
    for n in range(out.shape[3] // width):
        f = n
        turned = relayed((f // ROW + core) % 2, (f % ROW - source + ROW) % ROW,
                         (feed % ROW - source + ROW) % ROW, (feed // ROW + core) % 2)
        at = slice(n * width, (n + 1) * width)
        took = at

        re, im = (arrived[source, part, :, took].astype(jnp.float32) for part in range(2))

        @pl.when(turned)
        def _():
            out[0, 0, :, at] = re.T
            out[0, 1, :, at] = -im.T

        @pl.when(jnp.logical_not(turned))
        def _():
            out[0, 0, :, at] = re
            out[0, 1, :, at] = im

        @pl.when(f == feed)
        def _():
            low, cut = slice(n * width, n * width + width // 2), width // 2
            out[0, 0, cut:, low] = re[:cut, cut:].T
            out[0, 1, cut:, low] = -im[:cut, cut:].T


def per_device(voltages, gains):
    chans, rows, _, time = voltages.shape
    feeds = rows * PLANES * CORES * PLACES
    block = feeds // PLACES
    owned = chans // (PLANES * CORES)
    arrived = pl.pallas_call(
        kernel,
        out_shape=pltpu.VMEM((owned, 2, block, feeds), jnp.bfloat16),
        in_specs=[pl.BlockSpec(memory_space=pltpu.HBM), pl.BlockSpec(memory_space=pltpu.VMEM)],
        out_specs=pl.BlockSpec(memory_space=pltpu.VMEM),
        scratch_shapes=[
            pltpu.VMEM((chans, rows, 2, time), jnp.int32),
            pltpu.VMEM((chans * rows, 2 * time), jnp.bfloat16),
            pltpu.VMEM((feeds, 2 * time), jnp.bfloat16),
            pltpu.VMEM((PLACES, 2, block, feeds // CORES), jnp.bfloat16),
            pltpu.SemaphoreType.DMA((chans,)),
            pltpu.SemaphoreType.DMA,
            pltpu.SemaphoreType.DMA((PLACES, PLANES)),
            pltpu.SemaphoreType.DMA,
            pltpu.SemaphoreType.DMA,
            pltpu.SemaphoreType.DMA,
            pltpu.SemaphoreType.DMA((ROW, PLACES)),
            pltpu.SemaphoreType.DMA,
        ],
        compiler_params=pltpu.CompilerParams(collective_id=0, has_side_effects=True, vmem_limit_bytes=45 * 2**20),
        name="x_engine",
    )(voltages, gains.transpose(0, 2, 1))
    spec = pl.BlockSpec((1, 2, block, feeds), lambda i: (i, 0, 0, 0))
    return pl.pallas_call(
        finish,
        out_shape=jax.ShapeDtypeStruct(arrived.shape, jnp.float32),
        grid=(owned,),
        in_specs=[pl.BlockSpec(memory_space=pltpu.VMEM)],
        out_specs=spec,
        compiler_params=pltpu.CompilerParams(vmem_limit_bytes=24 * 2**20),
        name="widen",
    )(arrived)


def solution(mesh):
    in_specs = (P(None, ("feed", "freq"), None, None), P(None, None, ("feed", "freq")))
    out_specs = P("freq", None, "feed", None)
    return jax.shard_map(
        per_device, mesh=mesh, in_specs=in_specs, out_specs=out_specs, check_vma=False
    )
```
